32 devices in a mesh: mem: 4 (over x, core), reg: 8 (over z, y).
Axes of the slice: x: 2, y: 2, z: 4, core: 2. Of those that a mesh axis runs over, the one named last changes fastest.
Arguments:
- profiles: bfloat16 [2048, 80, 127], P('reg', 'mem'), may hold values from -6 to 6
- jacobian: bfloat16 [2048, 16, 127], P('reg'), may hold values from -0.5 to 0.5
- departure: float32 [32768], P('reg'), may hold values from -6 to 6
- obs_rinv: float32 [32768], P('reg'), may hold values from 0.1 to 2
- obs_level: int32 [32768], P('reg'), may hold values from 0 to 126
- vertical_modes: float32 [127, 12], replicated, may hold values from -2 to 2
- send_rows: int32 [8, 7, 512], P('reg'), may hold values from -1 to 4095, as said below
- counts: int32 [8, 7], P('reg'), may hold values from 64 to 512, as said below
- loc_taper: float32 [8, 7, 512], P('reg'), may hold values from 0.05 to 1
Outputs:
- gram_matrices: float32 [8, 960, 960], P('reg', 'mem')
- weighted_departures: float32 [8, 960], P('reg', 'mem')
The draws below stay inside these ranges and needn't reach their ends.
Inputs may be any that keep to these rules, and one draw needn't show every extreme that they name: counts[s, d] of the 512 slots that owner s sends to region (s + d - 3) mod 8 are live, the first ones; in every draw one region has all 512 slots live from each of its 7 owners. `send_rows`: a live slot holds a row of the owner's 4096 observations, no row twice within one (s, d); the other slots hold -1.
All inputs are finite; a program needn't handle non-finite values.
Results may differ from the reference program's by a relative error of at most 0.0095.
Values may be sent and summed in bfloat16 or wider, within the bound.
A program may use at most 64 MiB of HBM per device.

```python
import math
import jax
import jax.numpy as jnp
from jax import lax

ENS = 80
MODES = 12
LEV = 127
CH = 16
HALF = 3
COLS = 256
CAP = 512
REGIONS = 8
NB = 7
OBS = 32768
COLS_ALL = 2048


def routing_tables(key):
    key_base = jax.random.fold_in(key, 11)
    key_density = jax.random.fold_in(key, 12)
    key_full = jax.random.fold_in(key, 13)
    key_rows = jax.random.fold_in(key, 14)
    base_count = jax.random.randint(key_base, (REGIONS, NB), CAP // 8, CAP // 2 + 1)
    density = jax.random.randint(key_density, (REGIONS,), 1, 4)
    source = jnp.arange(REGIONS, dtype=jnp.int32)[:, None]
    offset = jnp.arange(NB, dtype=jnp.int32)[None, :]
    target = (source + offset - HALF) % REGIONS
    count_table = jnp.minimum(base_count * density[target], CAP)
    full_region = jax.random.randint(key_full, (), 0, REGIONS)
    count_table = jnp.where(target == full_region, CAP, count_table).astype(jnp.int32)
    row_keys = jax.random.split(key_rows, REGIONS * NB)
    orders = jax.vmap(lambda single: jax.random.permutation(single, COLS * CH)[:CAP])(row_keys)
    orders = orders.reshape(REGIONS, NB, CAP).astype(jnp.int32)
    slot_ids = jnp.arange(CAP, dtype=jnp.int32)[None, None, :]
    listed = jnp.where(slot_ids < count_table[:, :, None], orders, -1).astype(jnp.int32)
    return (listed, count_table)


def draw_send_rows(key, part):
    listed, count_table = routing_tables(key)
    return listed


def draw_counts(key, part):
    listed, count_table = routing_tables(key)
    return count_table


def plant(array, stream_key, smallest, high):
    spot = [jax.random.randint(jax.random.fold_in(stream_key, axis), (), 0, length) for axis, length in enumerate(array.shape)]
    widest = array.shape.index(max(array.shape))
    beside = spot[:widest] + [(spot[widest] + 1) % array.shape[widest]] + spot[widest + 1:]
    return array.at[tuple(spot)].set(smallest).at[tuple(beside)].set(high)


def level_of(stream_key, dims, cuts, least, largest):
    factor_of = 1.0
    for dim, shards_of in cuts:
        steps = jax.random.uniform(jax.random.fold_in(jax.random.fold_in(stream_key, 6), dim), (shards_of,), jnp.float32, least / len(cuts), largest / len(cuts))
        factor_of = factor_of * jnp.repeat(jnp.exp(steps), dims[dim] // shards_of).reshape((-1,) + (1,) * (len(dims) - 1 - dim))
    return factor_of


def noise(rng, dims, deviation, most, shards=(), kind=jnp.bfloat16):
    result = jax.random.normal(rng, dims, jnp.float32) * deviation
    if len(shards) > 0:
        result = level_of(rng, dims, shards, -0.22, 0.18) * result
    return jnp.clip(result, min=-most, max=most).astype(kind)


def setup_inputs(seed: int = 0) -> dict:
    seeds = jax.random.split(jax.random.key(seed), 10)
    profiles = noise(seeds[0], (COLS_ALL, ENS, LEV), 1.0, 6.0, ((0, 8), (1, 4)))
    jacobian = noise(seeds[1], (COLS_ALL, CH, LEV), LEV ** -0.5, 0.5, ((0, 8),))
    departure = noise(seeds[2], (OBS,), 1.0, 6.0, ((0, 8),), jnp.float32)
    obs_rinv = jnp.clip(jnp.exp(math.log(2.0) - 2.9957323 * jax.random.uniform(seeds[3], (OBS,), jnp.float32) ** level_of(seeds[3], (OBS,), ((0, 8),), -0.2, 0.2)), 0.1, 2.0)
    obs_level = plant(jax.random.randint(seeds[4], (OBS,), 0, LEV), jax.random.fold_in(seeds[4], 1), 0, LEV - 1).astype(jnp.int32)
    vertical_modes = noise(seeds[5], (LEV, MODES), 0.3, 2.0, (), jnp.float32)
    send_rows = draw_send_rows(jax.random.fold_in(seeds[9], 71), 0)
    counts = draw_counts(jax.random.fold_in(seeds[9], 71), 0)
    loc_taper = jnp.clip(0.05 + 0.95 * jax.random.uniform(seeds[8], (REGIONS, NB, CAP), jnp.float32) ** level_of(seeds[8], (REGIONS, NB, CAP), ((0, 8),), -0.2, 0.2), 0.05, 1.0)
    return {"profiles": profiles, "jacobian": jacobian, "departure": departure, "obs_rinv": obs_rinv, "obs_level": obs_level, "vertical_modes": vertical_modes, "send_rows": send_rows, "counts": counts, "loc_taper": loc_taper}


def reference(profiles, jacobian, departure, obs_rinv, obs_level, vertical_modes, send_rows, counts, loc_taper):
    profile_blocks = profiles.reshape(REGIONS, COLS, ENS, LEV)
    jacob_blocks = jacobian.reshape(REGIONS, COLS, CH, LEV)

    def owner_pert(operands):
        profile_one, jacob_one = operands
        values = jnp.einsum('cql,cml->mcq', jacob_one.astype(jnp.float32), profile_one.astype(jnp.float32), precision=lax.Precision.HIGHEST)
        return values.reshape(ENS, COLS * CH).astype(jnp.bfloat16)

    all_pert = lax.map(owner_pert, (profile_blocks, jacob_blocks))
    all_pert = jnp.transpose(all_pert, (1, 0, 2)).reshape(ENS, REGIONS * COLS * CH)
    factor = (ENS - 1) ** -0.5
    offsets = jnp.arange(NB, dtype=jnp.int32)
    slot_ids = jnp.arange(CAP, dtype=jnp.int32)

    def one_region(region):
        source = (region - offsets + HALF) % REGIONS
        listed = send_rows[source, offsets]
        live_slot = slot_ids[None, :] < counts[source, offsets][:, None]
        picked = jnp.where(live_slot, listed, 0)
        global_ids = (source[:, None] * (COLS * CH) + picked).reshape(-1)
        weight32 = jnp.where(live_slot, obs_rinv[global_ids].reshape(NB, CAP) * loc_taper[source, offsets], 0.0).reshape(-1)
        weight = weight32.astype(jnp.bfloat16)
        dep_weighted = (weight32 * departure[global_ids]).astype(jnp.bfloat16)
        mode_values = (vertical_modes[obs_level[global_ids]].T * factor).astype(jnp.bfloat16)
        region_pert = all_pert[:, global_ids]
        modulated = (region_pert.astype(jnp.float32)[:, None, :] * mode_values.astype(jnp.float32)[None, :, :]).astype(jnp.bfloat16)
        modulated = modulated.reshape(ENS * MODES, NB * CAP)
        weighted = (modulated.astype(jnp.float32) * weight.astype(jnp.float32)[None, :]).astype(jnp.bfloat16)
        gram_block = jnp.dot(modulated.astype(jnp.float32), weighted.astype(jnp.float32).T, precision=lax.Precision.HIGHEST)
        dep_block = jnp.dot(modulated.astype(jnp.float32), dep_weighted.astype(jnp.float32), precision=lax.Precision.HIGHEST)
        return gram_block, dep_block

    gram_matrices, weighted_departures = lax.map(one_region, jnp.arange(REGIONS, dtype=jnp.int32))
    return (gram_matrices, weighted_departures)
```

```python
import functools

import jax
import jax.numpy as jnp
from jax import lax
from jax.experimental import pallas as pl
from jax.experimental.pallas import tpu as pltpu
from jax.sharding import PartitionSpec as P

ENS = 80
ROWS = 32
GROUP = 8
LO = 512
NT = (((1,), (1,)), ((), ()))
VMEM = pl.BlockSpec(memory_space=pltpu.VMEM)
SMEM = pl.BlockSpec(memory_space=pltpu.SMEM)
MESH = pl.DeviceIdType.MESH


def iota(shape, dim):
    return lax.broadcasted_iota(jnp.int32, shape, dim)


def split3(x):
    hi = x.astype(jnp.bfloat16).astype(jnp.float32)
    rest = x - hi
    mid = rest.astype(jnp.bfloat16).astype(jnp.float32)
    return hi, mid, rest - mid


def pick_kernel(
    prof, jac, dep, rinv, level, modes, rows, counts, taper, out, stack, extra, table, side, block
):
    cols, members, levels = prof.shape
    channels = jac.shape[1]
    blocks, capacity = rows.shape[1], rows.shape[2]
    lanes = GROUP * channels
    share = side.shape[0] // lax.axis_size("mem")
    me = lax.axis_index("mem")

    extra[...] = jnp.zeros_like(extra)
    for first, source in ((0, rinv), (3, dep)):
        for step, part in enumerate(split3(source[...])):
            extra[first + step : first + step + 1, :] = part
    extra[6:7, :] = level[...].astype(jnp.float32)

    lane_col = iota((ROWS, lanes), 1) // channels
    is_member = iota((ROWS, lanes), 0) < members

    def fill(hi, carry):
        for part in range(LO // lanes):
            group = hi * (LO // lanes) + part
            base = group * GROUP
            for c in range(GROUP):
                start = pl.multiple_of((base + c) * ROWS, ROWS)
                stack[pl.ds(start, members), :] = prof[base + c]
            left = stack[pl.ds(pl.multiple_of(base * ROWS, ROWS * GROUP), ROWS * GROUP), :]
            right = jac[pl.ds(base, GROUP)].reshape(lanes, levels)
            full = lax.dot_general(left, right, NT, preferred_element_type=jnp.float32)
            acc = jnp.zeros((ROWS, lanes), jnp.float32)
            for c in range(GROUP):
                keep = (lane_col == c) & is_member
                acc = jnp.where(keep, full[c * ROWS : (c + 1) * ROWS], acc)
            tail = extra[:, pl.ds(pl.multiple_of(group * lanes, lanes), lanes)]
            whole = jnp.concatenate([acc[: ROWS - 8], tail], axis=0)
            table[hi, :, part * lanes : (part + 1) * lanes] = whole.astype(jnp.bfloat16)
        return carry

    his = table.shape[0]
    lax.fori_loop(0, his, fill, 0)

    scaled = (modes[...] * ((ENS - 1) ** (-0.5))).astype(jnp.bfloat16)
    kinds = scaled.shape[1]
    side[...] = jnp.zeros_like(side)
    block[...] = jnp.zeros_like(block)
    for d in range(blocks):
        live = iota((1, capacity), 1) < counts[0, d]
        picked = jnp.where(live, rows[0, d : d + 1, :], 0)
        high, low = picked // LO, picked % LO
        hot = jnp.where(iota((LO, capacity), 0) == low, 1.0, 0.0).astype(jnp.bfloat16)
        found = jnp.dot(
            table[...].reshape(his * ROWS, LO), hot, preferred_element_type=jnp.float32
        )
        chosen = jnp.where(high == 0, found[:ROWS], 0.0)
        for h in range(1, his):
            chosen = jnp.where(high == h, found[h * ROWS : (h + 1) * ROWS], chosen)
        slot_rinv = chosen[24:25] + chosen[25:26] + chosen[26:27]
        slot_dep = chosen[27:28] + chosen[28:29] + chosen[29:30]
        slot_level = chosen[30:31].astype(jnp.int32)
        weight32 = jnp.where(live, slot_rinv * taper[0, d : d + 1, :], 0.0)
        level_hot = jnp.where(iota((levels, capacity), 0) == slot_level, 1.0, 0.0)
        side[0:1, :] = weight32
        side[1:2, :] = weight32 * slot_dep
        side[2 : 2 + kinds, :] = lax.dot_general(
            scaled,
            level_hot.astype(jnp.bfloat16),
            (((0,), (0,)), ((), ())),
            preferred_element_type=jnp.float32,
        )
        block[0:24, :] = chosen[0:24]
        for j in range(side.shape[0] // share):

            @pl.when(me == j)
            def _():
                block[members : members + share, :] = side[j * share : (j + 1) * share, :]

        out[d] = block[...].astype(jnp.bfloat16)


def share_kernel(mine, region, s_reg, r_reg, s_x, r_x, s_p, r_p, s_q, r_q, here):
    blocks = mine.shape[0]
    middle = blocks // 2
    n_mem, n_reg = lax.axis_size("mem"), lax.axis_size("reg")
    me, reg = lax.axis_index("mem"), lax.axis_index("reg")
    chips = n_mem // 2
    twin = me + 1 - 2 * (me % 2)
    order = [middle]
    for far in range(1, middle + 1):
        order += [middle - far, middle + far]

    def to_reg(d):
        return {"mem": me, "reg": lax.rem(reg + d - middle + n_reg, n_reg)}

    def peer(j):
        return {"mem": lax.rem(me + 2 * j, n_mem), "reg": reg}

    partner = {"mem": twin, "reg": reg}
    barrier = pltpu.get_barrier_semaphore()
    greeted = [to_reg(d) for d in order[1:]] + [partner] + [peer(j) for j in range(1, chips)]
    for device in greeted:
        pl.semaphore_signal(barrier, inc=1, device_id=device, device_id_type=MESH)
    own = pltpu.make_async_copy(mine.at[middle], region.at[middle, me], here)
    own.start()
    pl.semaphore_wait(barrier, len(greeted))

    def remote(src, dst, send, recv, device):
        return pltpu.make_async_remote_copy(
            src_ref=src, dst_ref=dst, send_sem=send, recv_sem=recv,
            device_id=device, device_id_type=MESH,
        )

    sends = []
    across = {}
    for d in order[1:]:
        across[d] = remote(mine.at[d], region.at[d, me], s_reg.at[d], r_reg.at[d], to_reg(d))
        across[d].start()
    hops = {}
    twins = []
    for d in order:
        src = mine.at[d]
        if d != middle:
            across[d].wait_recv()
            src = region.at[d, me]
        for j in range(1, chips):
            hops[d, j] = remote(
                src, region.at[d, me], s_x.at[d, j], r_x.at[d, j], peer(j)
            )
            hops[d, j].start()
        copy = remote(src, region.at[d, me], s_p.at[d], r_p.at[d], partner)
        copy.start()
        twins.append(copy)
    for d in order:
        for j in range(1, chips):
            hops[d, j].wait_recv()
            theirs = lax.rem(me - 2 * j + n_mem, n_mem)
            at = region.at[d, theirs]
            copy = remote(at, at, s_q.at[d, j], r_q.at[d, j], partner)
            copy.start()
            twins.append(copy)
    for copy in twins:
        copy.wait_recv()
    for copy in list(across.values()) + list(hops.values()) + twins:
        copy.wait_send()
    own.wait()


def gram_kernel(members, kinds, share, region, gram, depart, weighted, dep_acc):
    blocks, height, capacity = region.shape
    n_mem = height // ROWS
    own = members * kinds
    me = lax.axis_index("mem")
    row = iota((own, height), 0)
    col = iota((own, height), 1)
    member = ((row.astype(jnp.float32) + 0.5) * (1.0 / kinds)).astype(jnp.int32)
    line = row - member * kinds + 2

    def hot(mask):
        return jnp.where(mask, 1.0, 0.0).astype(jnp.bfloat16)

    spread = [hot(col == member + j * ROWS) for j in range(n_mem)]
    spread_own = hot(col == member + me * ROWS)
    mode_at = (line // share) * ROWS + members + line % share
    spread_mode = hot(col == mode_at)
    gram[...] = jnp.zeros_like(gram)
    dep_acc[...] = jnp.zeros_like(dep_acc)

    def times(left, right):
        return jnp.dot(left, right, preferred_element_type=jnp.float32)

    def step(d, carry):
        data = region[d]
        mode = times(spread_mode, data)
        top = data[16:32].astype(jnp.float32)
        weight = top[members - 16 : members - 15]
        dep = top[members - 15 : members - 14]
        z_own = (times(spread_own, data) * mode).astype(jnp.bfloat16)
        for j in range(n_mem):
            z = (times(spread[j], data) * mode).astype(jnp.bfloat16)
            weighted[j * own : (j + 1) * own, :] = (z.astype(jnp.float32) * weight).astype(
                jnp.bfloat16
            )
        gram[0] += lax.dot_general(z_own, weighted[...], NT, preferred_element_type=jnp.float32)
        dep8 = jnp.broadcast_to(dep, (16, capacity)).astype(jnp.bfloat16)
        dep_acc[...] += lax.dot_general(dep8, z_own, NT, preferred_element_type=jnp.float32)
        return carry

    lax.fori_loop(0, blocks, step, 0)
    depart[...] = dep_acc[0:1, :]


def local(
    profiles, jacobian, departure, obs_rinv, obs_level, vertical_modes, send_rows, counts, loc_taper
):
    cols, members, levels = profiles.shape
    channels = jacobian.shape[1]
    blocks, capacity = send_rows.shape[1], send_rows.shape[2]
    kinds = vertical_modes.shape[1]
    n_mem = lax.axis_size("mem")
    chips = n_mem // 2
    obs = cols * channels
    share = -(-(kinds + 2) // n_mem)
    mine = pl.pallas_call(
        pick_kernel,
        out_shape=jax.ShapeDtypeStruct((blocks, ROWS, capacity), jnp.bfloat16),
        in_specs=[VMEM] * 7 + [SMEM, VMEM],
        out_specs=VMEM,
        scratch_shapes=[
            pltpu.VMEM((cols * ROWS, levels), jnp.bfloat16),
            pltpu.VMEM((8, obs), jnp.float32),
            pltpu.VMEM((obs // LO, ROWS, LO), jnp.bfloat16),
            pltpu.VMEM((share * n_mem, capacity), jnp.float32),
            pltpu.VMEM((ROWS, capacity), jnp.float32),
        ],
        name="pick",
    )(
        profiles, jacobian, departure[None], obs_rinv[None], obs_level[None], vertical_modes,
        send_rows, counts, loc_taper,
    )
    dma = pltpu.SemaphoreType.DMA
    region = pl.pallas_call(
        share_kernel,
        out_shape=jax.ShapeDtypeStruct((blocks, n_mem, ROWS, capacity), jnp.bfloat16),
        in_specs=[VMEM],
        out_specs=VMEM,
        scratch_shapes=[dma((blocks,)), dma((blocks,)), dma((blocks, chips)), dma((blocks, chips)),
                        dma((blocks,)), dma((blocks,)), dma((blocks, chips)), dma((blocks, chips)),
                        dma],
        compiler_params=pltpu.CompilerParams(collective_id=0, has_side_effects=True),
        name="share",
    )(mine)
    own = members * kinds
    gram, depart = pl.pallas_call(
        functools.partial(gram_kernel, members, kinds, share),
        out_shape=(
            jax.ShapeDtypeStruct((1, own, own * n_mem), jnp.float32),
            jax.ShapeDtypeStruct((1, own), jnp.float32),
        ),
        in_specs=[VMEM],
        out_specs=(VMEM, VMEM),
        scratch_shapes=[
            pltpu.VMEM((own * n_mem, capacity), jnp.bfloat16),
            pltpu.VMEM((16, own), jnp.float32),
        ],
        name="gram",
    )(region.reshape(blocks, n_mem * ROWS, capacity))
    return gram, depart


def solution(mesh):
    in_specs = (
        P("reg", "mem", None),
        P("reg", None, None),
        P("reg"),
        P("reg"),
        P("reg"),
        P(),
        P("reg", None, None),
        P("reg", None),
        P("reg", None, None),
    )
    out_specs = (P("reg", "mem", None), P("reg", "mem"))
    return jax.shard_map(local, mesh=mesh, in_specs=in_specs, out_specs=out_specs, check_vma=False)
```

```python
import functools

import jax
import jax.numpy as jnp
from jax import lax
from jax.experimental import pallas as pl
from jax.experimental.pallas import tpu as pltpu
from jax.sharding import PartitionSpec as P

ENS = 80
LANE = 128
GROUP = 16
NT = (((1,), (1,)), ((), ()))
VMEM = pl.BlockSpec(memory_space=pltpu.VMEM)
SMEM = pl.BlockSpec(memory_space=pltpu.SMEM)
MESH = pl.DeviceIdType.MESH
LAG = 2


def iota(shape, dim):
    return lax.broadcasted_iota(jnp.int32, shape, dim)


def hot(mask):
    return jnp.where(mask, 1.0, 0.0).astype(jnp.bfloat16)


def times(left, right):
    return jnp.dot(left, right, preferred_element_type=jnp.float32)


def split3(x):
    hi = x.astype(jnp.bfloat16).astype(jnp.float32)
    rest = x - hi
    mid = rest.astype(jnp.bfloat16).astype(jnp.float32)
    return hi, mid, rest - mid


def pick_kernel(
    prof, jac, dep, rinv, level, modes, rows, counts, taper,
    out, wide, turned, extra, table, side, block,
):
    members, cols, levels = prof.shape
    channels = jac.shape[1]
    blocks, capacity = rows.shape[0], rows.shape[2]
    lanes = GROUP * channels
    his, height = table.shape[0], table.shape[1]
    share = side.shape[0] // lax.axis_size("mem")
    me = lax.axis_index("mem")

    depth = wide.shape[1] // channels
    for half in range(cols // LANE):
        part = jac[:, :, half * LANE : (half + 1) * LANE].reshape(levels * channels, LANE)
        wide[half, 0 : levels * channels, :] = part.astype(jnp.float32)
        for q in range(channels):
            plane = wide[half, pl.ds(q, depth, stride=channels), :]
            turned[q, half * LANE : (half + 1) * LANE, :] = plane.T[:, :levels].astype(jnp.bfloat16)

    extra[...] = jnp.zeros_like(extra)
    parts = split3(rinv[...]) + split3(dep[...]) + (level[...].astype(jnp.float32),)
    for k, part in enumerate(parts):
        for g in range(his):
            extra[g * 8 + k : g * 8 + k + 1, :] = part[:, g * lanes : (g + 1) * lanes]
    source, target = iota((lanes, lanes), 0), iota((lanes, lanes), 1)
    swap = hot(target == (source % channels) * GROUP + source // channels)
    extra[...] = times(extra[...].astype(jnp.bfloat16), swap)

    tall = members * GROUP
    diagonal = iota((tall, lanes), 0) % GROUP == iota((tall, lanes), 1) % GROUP
    fold = hot(iota((height, tall), 0) == iota((height, tall), 1) // GROUP)

    def fill(g, carry):
        first = pl.ds(pl.multiple_of(g * GROUP, GROUP), GROUP)
        left = prof[:, first, :].reshape(tall, levels)
        right = turned[:, first, :].reshape(lanes, levels)
        full = lax.dot_general(left, right, NT, preferred_element_type=jnp.float32)
        kept = jnp.where(diagonal, full, 0.0).astype(jnp.bfloat16)
        tail = extra[pl.ds(pl.multiple_of(g * 8, 8), 8), :]
        whole = jnp.concatenate([times(fold, kept)[: height - 8], tail], axis=0)
        table[g] = whole.astype(jnp.bfloat16)
        return carry

    lax.fori_loop(0, his, fill, 0, unroll=4)

    scaled = (modes[...] * ((ENS - 1) ** (-0.5))).astype(jnp.bfloat16)
    kinds = scaled.shape[0]
    side[...] = jnp.zeros_like(side)
    for d in range(blocks):
        live = iota((1, capacity), 1) < counts[0, d]
        picked = jnp.where(live, rows[d], 0)
        high = picked // lanes
        low = (picked % channels) * GROUP + (picked // channels) % GROUP
        found = times(
            table[...].reshape(his * height, lanes), hot(iota((lanes, capacity), 0) == low)
        )
        chosen = jnp.where(high == 0, found[:height], 0.0)
        for h in range(1, his):
            chosen = jnp.where(high == h, found[h * height : (h + 1) * height], chosen)
        x = height - 8
        slot_rinv = chosen[x : x + 1] + chosen[x + 1 : x + 2] + chosen[x + 2 : x + 3]
        slot_dep = chosen[x + 3 : x + 4] + chosen[x + 4 : x + 5] + chosen[x + 5 : x + 6]
        slot_level = chosen[x + 6 : x + 7].astype(jnp.int32)
        weight32 = jnp.where(live, slot_rinv * taper[d], 0.0)
        side[0:1, :] = weight32
        side[1:2, :] = weight32 * slot_dep
        side[2 : 2 + kinds, :] = times(scaled, hot(iota((levels, capacity), 0) == slot_level))
        block[0:members, :] = chosen[0:members]
        for j in range(side.shape[0] // share):

            @pl.when(me == j)
            def _():
                block[members : members + share, :] = side[j * share : (j + 1) * share, :]

        out[d] = block[...].astype(jnp.bfloat16)


def gram_kernel(
    members, kinds, share, mine, gram, depart,
    region, plain, weighted, dep_acc, s_reg, r_reg, s_x, r_x, s_p, r_p, s_q, r_q, here,
):
    blocks, height, capacity = mine.shape
    middle = blocks // 2
    n_mem, n_reg = lax.axis_size("mem"), lax.axis_size("reg")
    me, reg = lax.axis_index("mem"), lax.axis_index("reg")
    chips = n_mem // 2
    partner = {"mem": me + 1 - 2 * (me % 2), "reg": reg}

    def turn(k):
        return middle + ((k + 1) // 2) * (1 - 2 * (k % 2))

    def to_reg(d):
        return {"mem": me, "reg": lax.rem(reg + d - middle + n_reg, n_reg)}

    def peer(j):
        return {"mem": lax.rem(me + 2 * j, n_mem), "reg": reg}

    def remote(src, dst, send, recv, device):
        return pltpu.make_async_remote_copy(
            src_ref=src, dst_ref=dst, send_sem=send, recv_sem=recv,
            device_id=device, device_id_type=MESH,
        )

    def across(d):
        return remote(mine.at[d], region.at[d, me], s_reg.at[d], r_reg.at[d], to_reg(d))

    def hop(d, j):
        at = region.at[d, me]
        return remote(at, at, s_x.at[d, j], r_x.at[d, j], peer(j))

    def hand(d):
        at = region.at[d, me]
        return remote(at, at, s_p.at[d], r_p.at[d], partner)

    def relay(d, j):
        at = region.at[d, lax.rem(me - 2 * j + n_mem, n_mem)]
        return remote(at, at, s_q.at[d, j], r_q.at[d, j], partner)

    barrier = pltpu.get_barrier_semaphore()
    greeted = [to_reg(turn(k)) for k in range(1, blocks)] + [partner]
    greeted += [peer(j) for j in range(1, chips)]
    for device in greeted:
        pl.semaphore_signal(barrier, inc=1, device_id=device, device_id_type=MESH)
    own = pltpu.make_async_copy(mine.at[middle], region.at[middle, me], here)
    own.start()
    gram[...] = jnp.zeros_like(gram)
    dep_acc[...] = jnp.zeros_like(dep_acc)
    size = members * kinds
    row, col = iota((size, height), 0), iota((size, height), 1)
    spread = hot(col == row // kinds)
    period = 4 * kinds
    line = iota((period, height), 0) % kinds + 2
    spot = iota((period, height), 1)
    spread_mode = [
        hot((line // share == j) & (spot == members + line % share)) for j in range(n_mem)
    ]
    pl.semaphore_wait(barrier, len(greeted))
    for k in range(1, blocks):
        across(turn(k)).start()
    own.wait()

    def forward(k):
        d = turn(k)

        @pl.when(k > 0)
        def _():
            across(d).wait_recv()

        for j in range(1, chips):
            hop(d, j).start()
        hand(d).start()

    def pass_on(k):
        d = turn(k)
        for j in range(1, chips):
            hop(d, j).wait_recv()
            relay(d, j).start()

    def multiply(k):
        d = turn(k)
        hand(d).wait_recv()
        for j in range(1, chips):
            relay(d, j).wait_recv()
        mode = times(spread_mode[0], region[d, 0])
        for j in range(1, n_mem):
            mode += times(spread_mode[j], region[d, j])
        mode = jnp.concatenate([mode] * (size // period), axis=0)
        rows = region[d, 0].astype(jnp.float32)
        weight, dep = rows[members : members + 1], rows[members + 1 : members + 2]
        for j in range(n_mem):
            z = (times(spread, region[d, j]) * mode).astype(jnp.bfloat16)
            plain[j] = z
            weighted[j * size : (j + 1) * size, :] = (z.astype(jnp.float32) * weight).astype(
                jnp.bfloat16
            )
        z_own = plain[me]
        gram[0] += lax.dot_general(z_own, weighted[...], NT, preferred_element_type=jnp.float32)
        dep16 = jnp.broadcast_to(dep, (16, capacity)).astype(jnp.bfloat16)
        dep_acc[...] += lax.dot_general(dep16, z_own, NT, preferred_element_type=jnp.float32)

    def step(k, carry):
        @pl.when(k < blocks)
        def _():
            forward(k)

        @pl.when((k >= LAG) & (k < blocks + LAG))
        def _():
            pass_on(k - LAG)

        @pl.when(k >= 2 * LAG)
        def _():
            multiply(k - 2 * LAG)

        return carry

    lax.fori_loop(0, blocks + 2 * LAG, step, 0)
    for k in range(blocks):
        d = turn(k)
        if k > 0:
            across(d).wait_send()
        hand(d).wait_send()
        for j in range(1, chips):
            hop(d, j).wait_send()
            relay(d, j).wait_send()
    depart[...] = dep_acc[0:1, :]


def local(
    profiles, jacobian, departure, obs_rinv, obs_level, vertical_modes, send_rows, counts, loc_taper
):
    cols, members, levels = profiles.shape
    channels = jacobian.shape[1]
    blocks, capacity = send_rows.shape[1], send_rows.shape[2]
    kinds = vertical_modes.shape[1]
    n_mem = lax.axis_size("mem")
    chips = n_mem // 2
    share = -(-(kinds + 2) // n_mem)
    height = members + share
    mine = pl.pallas_call(
        pick_kernel,
        out_shape=jax.ShapeDtypeStruct((blocks, height, capacity), jnp.bfloat16),
        in_specs=[VMEM] * 7 + [SMEM, VMEM],
        out_specs=VMEM,
        scratch_shapes=[
            pltpu.VMEM((cols // LANE, -(-levels // LANE) * LANE * channels, LANE), jnp.float32),
            pltpu.VMEM((channels, cols, levels), jnp.bfloat16),
            pltpu.VMEM((cols // GROUP * 8, GROUP * channels), jnp.float32),
            pltpu.VMEM((cols // GROUP, 32, GROUP * channels), jnp.bfloat16),
            pltpu.VMEM((share * n_mem, capacity), jnp.float32),
            pltpu.VMEM((height, capacity), jnp.float32),
        ],
        name="pick",
    )(
        profiles.transpose(1, 0, 2), jacobian.transpose(2, 1, 0),
        departure[None], obs_rinv[None], obs_level[None], vertical_modes.T,
        send_rows.transpose(1, 0, 2), counts, loc_taper.transpose(1, 0, 2),
    )
    dma = pltpu.SemaphoreType.DMA
    own = members * kinds
    one, two = dma((blocks,)), dma((blocks, chips))
    gram, depart = pl.pallas_call(
        functools.partial(gram_kernel, members, kinds, share),
        out_shape=(
            jax.ShapeDtypeStruct((1, own, own * n_mem), jnp.float32),
            jax.ShapeDtypeStruct((1, own), jnp.float32),
        ),
        in_specs=[VMEM],
        out_specs=(VMEM, VMEM),
        scratch_shapes=[
            pltpu.VMEM((blocks, n_mem, height, capacity), jnp.bfloat16),
            pltpu.VMEM((n_mem, own, capacity), jnp.bfloat16),
            pltpu.VMEM((own * n_mem, capacity), jnp.bfloat16),
            pltpu.VMEM((16, own), jnp.float32),
            one, one, two, two, one, one, two, two, dma,
        ],
        compiler_params=pltpu.CompilerParams(collective_id=0, has_side_effects=True),
        name="gram",
    )(mine)
    return gram, depart


def solution(mesh):
    in_specs = (
        P("reg", "mem", None),
        P("reg", None, None),
        P("reg"),
        P("reg"),
        P("reg"),
        P(),
        P("reg", None, None),
        P("reg", None),
        P("reg", None, None),
    )
    out_specs = (P("reg", "mem", None), P("reg", "mem"))
    return jax.shard_map(local, mesh=mesh, in_specs=in_specs, out_specs=out_specs, check_vma=False)
```

```python
import functools

import jax
import jax.numpy as jnp
from jax import lax
from jax.experimental import pallas as pl
from jax.experimental.pallas import tpu as pltpu
from jax.sharding import PartitionSpec as P

ENS = 80
LANE = 128
GROUP = 16
NT = (((1,), (1,)), ((), ()))
VMEM = pl.BlockSpec(memory_space=pltpu.VMEM)
SMEM = pl.BlockSpec(memory_space=pltpu.SMEM)
MESH = pl.DeviceIdType.MESH
LAG = 2


def iota(shape, dim):
    return lax.broadcasted_iota(jnp.int32, shape, dim)


def hot(mask):
    return jnp.where(mask, 1.0, 0.0).astype(jnp.bfloat16)


def times(left, right):
    return jnp.dot(left, right, preferred_element_type=jnp.float32)


def split3(x):
    hi = x.astype(jnp.bfloat16).astype(jnp.float32)
    rest = x - hi
    mid = rest.astype(jnp.bfloat16).astype(jnp.float32)
    return hi, mid, rest - mid


def pick(
    order, ready, prof, jac, dep, rinv, level, modes, rows, counts, taper,
    out, wide, turned, extra, table, side, block,
):
    members, cols, levels = prof.shape
    channels = jac.shape[1]
    blocks, capacity = rows.shape[0], rows.shape[2]
    lanes = GROUP * channels
    his, height = table.shape[0], table.shape[1]
    share = side.shape[0] // lax.axis_size("mem")
    me = lax.axis_index("mem")

    depth = wide.shape[1] // channels
    for half in range(cols // LANE):
        part = jac[:, :, half * LANE : (half + 1) * LANE].reshape(levels * channels, LANE)
        wide[half, 0 : levels * channels, :] = part.astype(jnp.float32)
        for q in range(channels):
            plane = wide[half, pl.ds(q, depth, stride=channels), :]
            turned[q, half * LANE : (half + 1) * LANE, :] = plane.T[:, :levels].astype(jnp.bfloat16)

    extra[...] = jnp.zeros_like(extra)
    parts = split3(rinv[...]) + split3(dep[...]) + (level[...].astype(jnp.float32),)
    for k, part in enumerate(parts):
        for g in range(his):
            extra[g * 8 + k : g * 8 + k + 1, :] = part[:, g * lanes : (g + 1) * lanes]
    source, target = iota((lanes, lanes), 0), iota((lanes, lanes), 1)
    swap = hot(target == (source % channels) * GROUP + source // channels)
    extra[...] = times(extra[...].astype(jnp.bfloat16), swap)

    tall = members * GROUP
    diagonal = iota((tall, lanes), 0) % GROUP == iota((tall, lanes), 1) % GROUP
    fold = hot(iota((height, tall), 0) == iota((height, tall), 1) // GROUP)

    def fill(g, carry):
        first = pl.ds(pl.multiple_of(g * GROUP, GROUP), GROUP)
        left = prof[:, first, :].reshape(tall, levels)
        right = turned[:, first, :].reshape(lanes, levels)
        full = lax.dot_general(left, right, NT, preferred_element_type=jnp.float32)
        kept = jnp.where(diagonal, full, 0.0).astype(jnp.bfloat16)
        tail = extra[pl.ds(pl.multiple_of(g * 8, 8), 8), :]
        whole = jnp.concatenate([times(fold, kept)[: height - 8], tail], axis=0)
        table[g] = whole.astype(jnp.bfloat16)
        return carry

    lax.fori_loop(0, his, fill, 0, unroll=4)

    scaled = (modes[...] * ((ENS - 1) ** (-0.5))).astype(jnp.bfloat16)
    kinds = scaled.shape[0]
    side[...] = jnp.zeros_like(side)
    for k, d in enumerate(order):
        live = iota((1, capacity), 1) < counts[0, d]
        picked = jnp.where(live, rows[d], 0)
        high = picked // lanes
        low = (picked % channels) * GROUP + (picked // channels) % GROUP
        found = times(
            table[...].reshape(his * height, lanes), hot(iota((lanes, capacity), 0) == low)
        )
        chosen = jnp.where(high == 0, found[:height], 0.0)
        for h in range(1, his):
            chosen = jnp.where(high == h, found[h * height : (h + 1) * height], chosen)
        x = height - 8
        slot_rinv = chosen[x : x + 1] + chosen[x + 1 : x + 2] + chosen[x + 2 : x + 3]
        slot_dep = chosen[x + 3 : x + 4] + chosen[x + 4 : x + 5] + chosen[x + 5 : x + 6]
        slot_level = chosen[x + 6 : x + 7].astype(jnp.int32)
        weight32 = jnp.where(live, slot_rinv * taper[d], 0.0)
        side[0:1, :] = weight32
        side[1:2, :] = weight32 * slot_dep
        side[2 : 2 + kinds, :] = times(scaled, hot(iota((levels, capacity), 0) == slot_level))
        block[0:members, :] = chosen[0:members]
        for j in range(side.shape[0] // share):

            @pl.when(me == j)
            def _():
                block[members : members + share, :] = side[j * share : (j + 1) * share, :]

        out[d] = block[...].astype(jnp.bfloat16)
        ready(k)


def gram_kernel(
    members, kinds, share, prof, jac, dep, rinv, level, modes, rows, counts, taper, gram, depart,
    wide, turned, extra, table, side, block, mine, region, plain, weighted, dep_acc, s_reg, r_reg, s_x, r_x, s_p, r_p, s_q, r_q,
):
    blocks, height, capacity = mine.shape
    middle = blocks // 2
    n_mem, n_reg = lax.axis_size("mem"), lax.axis_size("reg")
    me, reg = lax.axis_index("mem"), lax.axis_index("reg")
    chips = n_mem // 2
    partner = {"mem": me + 1 - 2 * (me % 2), "reg": reg}

    def turn(k):
        k = blocks - 1 - k
        return middle + ((k + 1) // 2) * (1 - 2 * (k % 2))

    def to_reg(d):
        return {"mem": me, "reg": lax.rem(reg + d - middle + n_reg, n_reg)}

    def peer(j):
        return {"mem": lax.rem(me + 2 * j, n_mem), "reg": reg}

    def remote(src, dst, send, recv, device):
        return pltpu.make_async_remote_copy(
            src_ref=src, dst_ref=dst, send_sem=send, recv_sem=recv,
            device_id=device, device_id_type=MESH,
        )

    def across(d):
        return remote(mine.at[d], region.at[d, me], s_reg.at[d], r_reg.at[d], to_reg(d))

    def hop(d, j):
        at = region.at[d, me]
        return remote(at, at, s_x.at[d, j], r_x.at[d, j], peer(j))

    def hand(d):
        at = region.at[d, me]
        return remote(at, at, s_p.at[d], r_p.at[d], partner)

    def relay(d, j):
        at = region.at[d, lax.rem(me - 2 * j + n_mem, n_mem)]
        return remote(at, at, s_q.at[d, j], r_q.at[d, j], partner)

    barrier = pltpu.get_barrier_semaphore()
    greeted = [to_reg(turn(k)) for k in range(blocks - 1)] + [partner]
    greeted += [peer(j) for j in range(1, chips)]
    for device in greeted:
        pl.semaphore_signal(barrier, inc=1, device_id=device, device_id_type=MESH)

    def ready(k):
        if k == blocks - 1:
            region[middle, me] = mine[middle]
        if k == 1:
            pl.semaphore_wait(barrier, len(greeted))
        if k > 0:
            across(turn(k - 1)).start()

    pick(
        [turn(k) for k in range(blocks)], ready, prof, jac, dep, rinv, level, modes, rows, counts,
        taper, mine, wide, turned, extra, table, side, block,
    )
    gram[...] = jnp.zeros_like(gram)
    dep_acc[...] = jnp.zeros_like(dep_acc)
    size = members * kinds
    row, col = iota((size, height), 0), iota((size, height), 1)
    spread = hot(col == row // kinds)
    period = 4 * kinds
    line = iota((period, height), 0) % kinds + 2
    spot = iota((period, height), 1)
    spread_mode = [
        hot((line // share == j) & (spot == members + line % share)) for j in range(n_mem)
    ]

    def forward(k):
        d = turn(k)

        @pl.when(k < blocks - 1)
        def _():
            across(d).wait_recv()

        for j in range(1, chips):
            hop(d, j).start()
        hand(d).start()

    def pass_on(k):
        d = turn(k)
        for j in range(1, chips):
            hop(d, j).wait_recv()
            relay(d, j).start()

    def multiply(k):
        d = turn(k)
        hand(d).wait_recv()
        for j in range(1, chips):
            relay(d, j).wait_recv()
        mode = times(spread_mode[0], region[d, 0])
        for j in range(1, n_mem):
            mode += times(spread_mode[j], region[d, j])
        mode = jnp.concatenate([mode] * (size // period), axis=0)
        first = region[d, 0].astype(jnp.float32)
        weight, depw = first[members : members + 1], first[members + 1 : members + 2]
        for j in range(n_mem):
            z = (times(spread, region[d, j]) * mode).astype(jnp.bfloat16)
            plain[j] = z
            weighted[j * size : (j + 1) * size, :] = (z.astype(jnp.float32) * weight).astype(
                jnp.bfloat16
            )
        z_own = plain[me]
        gram[0] += lax.dot_general(z_own, weighted[...], NT, preferred_element_type=jnp.float32)
        dep16 = jnp.broadcast_to(depw, (16, capacity)).astype(jnp.bfloat16)
        dep_acc[...] += lax.dot_general(dep16, z_own, NT, preferred_element_type=jnp.float32)

    def step(k, carry):
        @pl.when(k < blocks)
        def _():
            forward(k)

        @pl.when((k >= LAG) & (k < blocks + LAG))
        def _():
            pass_on(k - LAG)

        @pl.when(k >= 2 * LAG)
        def _():
            multiply(k - 2 * LAG)

        return carry

    lax.fori_loop(0, blocks + 2 * LAG, step, 0)
    for k in range(blocks):
        d = turn(k)
        if k < blocks - 1:
            across(d).wait_send()
        hand(d).wait_send()
        for j in range(1, chips):
            hop(d, j).wait_send()
            relay(d, j).wait_send()
    depart[...] = dep_acc[0:1, :]


def local(
    profiles, jacobian, departure, obs_rinv, obs_level, vertical_modes, send_rows, counts, loc_taper
):
    cols, members, levels = profiles.shape
    channels = jacobian.shape[1]
    blocks, capacity = send_rows.shape[1], send_rows.shape[2]
    kinds = vertical_modes.shape[1]
    n_mem = lax.axis_size("mem")
    chips = n_mem // 2
    share = -(-(kinds + 2) // n_mem)
    height = members + share
    dma = pltpu.SemaphoreType.DMA
    own = members * kinds
    one, two = dma((blocks,)), dma((blocks, chips))
    gram, depart = pl.pallas_call(
        functools.partial(gram_kernel, members, kinds, share),
        out_shape=(
            jax.ShapeDtypeStruct((1, own, own * n_mem), jnp.float32),
            jax.ShapeDtypeStruct((1, own), jnp.float32),
        ),
        in_specs=[VMEM] * 7 + [SMEM, VMEM],
        out_specs=(VMEM, VMEM),
        scratch_shapes=[
            pltpu.VMEM((cols // LANE, -(-levels // LANE) * LANE * channels, LANE), jnp.float32),
            pltpu.VMEM((channels, cols, levels), jnp.bfloat16),
            pltpu.VMEM((cols // GROUP * 8, GROUP * channels), jnp.float32),
            pltpu.VMEM((cols // GROUP, 32, GROUP * channels), jnp.bfloat16),
            pltpu.VMEM((share * n_mem, capacity), jnp.float32),
            pltpu.VMEM((height, capacity), jnp.float32),
            pltpu.VMEM((blocks, height, capacity), jnp.bfloat16),
            pltpu.VMEM((blocks, n_mem, height, capacity), jnp.bfloat16),
            pltpu.VMEM((n_mem, own, capacity), jnp.bfloat16),
            pltpu.VMEM((own * n_mem, capacity), jnp.bfloat16),
            pltpu.VMEM((16, own), jnp.float32),
            one, one, two, two, one, one, two, two,
        ],
        compiler_params=pltpu.CompilerParams(collective_id=0, has_side_effects=True),
        name="gram",
    )(
        profiles.transpose(1, 0, 2), jacobian.transpose(2, 1, 0),
        departure[None], obs_rinv[None], obs_level[None], vertical_modes.T,
        send_rows.transpose(1, 0, 2), counts, loc_taper.transpose(1, 0, 2),
    )
    return gram, depart


def solution(mesh):
    in_specs = (
        P("reg", "mem", None),
        P("reg", None, None),
        P("reg"),
        P("reg"),
        P("reg"),
        P(),
        P("reg", None, None),
        P("reg", None),
        P("reg", None, None),
    )
    out_specs = (P("reg", "mem", None), P("reg", "mem"))
    return jax.shard_map(local, mesh=mesh, in_specs=in_specs, out_specs=out_specs, check_vma=False)
```
